8 devices in a mesh: dp: 1 (over z), tp: 8 (over y, x, core).
Axes of the slice: x: 2, y: 2, z: 1, core: 2. Of those that a mesh axis runs over, the one named last changes fastest.
Arguments:
- tokens_in: bfloat16 [48, 768, 2048], P('dp')
- ln_gain: float32 [2048], replicated
- ln_bias: float32 [2048], replicated
- w_qkv: bfloat16 [2048, 16, 384], P(None, 'tp')
- w_out: bfloat16 [2048, 2048], P('tp')
- w_up: bfloat16 [2048, 8192], P(None, 'tp')
- w_down: bfloat16 [8192, 2048], P('tp')
- grad_out: bfloat16 [48, 768, 2048], P('dp')
Outputs:
- output 1: bfloat16 [48, 768, 2048], P('dp')
- output 2: bfloat16 [2048, 16, 384], P('dp', 'tp')
- output 3: bfloat16 [2048, 2048], P(('dp', 'tp'))
- output 4: bfloat16 [2048, 8192], P('dp', 'tp')
- output 5: bfloat16 [8192, 2048], P(('dp', 'tp'))
All inputs are finite; a program needn't handle non-finite values.
Results may differ from the reference program's by a relative error of at most 0.0091197.
Values are sent between devices in bfloat16 or wider.
A program may use at most 2 GiB of HBM per device.

```python
import jax
import jax.numpy as jnp
from jax import lax

GROUP_ROWS = 48
SEQ_LEN = 768
DMODEL = 2048
FFN_DIM = 8192
Q_HEADS = 16
KV_HEADS = 16
HEAD_DIM = 128

LN_EPS = 1e-5
GELU_COEF = 0.7071067811865476
PDF_COEF = 0.3989422804014327
Q_PER_GROUP = Q_HEADS // KV_HEADS
GROUP_COLS = (Q_PER_GROUP + 2) * HEAD_DIM


def setup_inputs(seed: int = 0, part: int = 0) -> dict:
    shared_keys = jax.random.split(jax.random.key(seed), 6)
    part_keys = jax.random.split(jax.random.fold_in(jax.random.key(seed + 1), part), 2)
    act_shape = (GROUP_ROWS, SEQ_LEN, DMODEL)
    tokens_in = jax.random.normal(part_keys[0], act_shape, jnp.float32).astype(jnp.bfloat16)
    grad_out = jax.random.normal(part_keys[1], act_shape, jnp.float32).astype(jnp.bfloat16)
    ln_gain = 1.0 + 0.3 * jax.random.normal(shared_keys[0], (DMODEL,), jnp.float32)
    ln_bias = 0.3 * jax.random.normal(shared_keys[1], (DMODEL,), jnp.float32)
    w_qkv = (jax.random.normal(shared_keys[2], (DMODEL, KV_HEADS, GROUP_COLS), jnp.float32) * DMODEL ** -0.5).astype(jnp.bfloat16)
    w_out = (jax.random.normal(shared_keys[3], (Q_HEADS * HEAD_DIM, DMODEL), jnp.float32) * (Q_HEADS * HEAD_DIM) ** -0.5).astype(jnp.bfloat16)
    w_up = (jax.random.normal(shared_keys[4], (DMODEL, FFN_DIM), jnp.float32) * DMODEL ** -0.5).astype(jnp.bfloat16)
    w_down = (jax.random.normal(shared_keys[5], (FFN_DIM, DMODEL), jnp.float32) * FFN_DIM ** -0.5).astype(jnp.bfloat16)
    return dict(tokens_in=tokens_in, ln_gain=ln_gain, ln_bias=ln_bias, w_qkv=w_qkv, w_out=w_out, w_up=w_up, w_down=w_down, grad_out=grad_out)


def attend_row(row_pair):
    qkv_row, dout_row = row_pair
    q_row = qkv_row[:, :, :Q_PER_GROUP].astype(jnp.float32)
    k_row = qkv_row[:, :, Q_PER_GROUP].astype(jnp.float32)
    v_row = qkv_row[:, :, Q_PER_GROUP + 1].astype(jnp.float32)
    dout_f32 = dout_row.astype(jnp.float32)
    score_scale = HEAD_DIM ** -0.5
    causal = jnp.arange(SEQ_LEN)[:, None] >= jnp.arange(SEQ_LEN)[None, :]
    scores = jnp.einsum('qgpd,kgd->gpqk', q_row, k_row) * score_scale
    soft_probs = jax.nn.softmax(jnp.where(causal, scores, -1e30), axis=-1)
    probs_bf = soft_probs.astype(jnp.bfloat16).astype(jnp.float32)
    attn_out = jnp.einsum('gpqk,kgd->qgpd', probs_bf, v_row).astype(jnp.bfloat16)
    d_probs = jnp.einsum('qgpd,kgd->gpqk', dout_f32, v_row)
    d_val = jnp.einsum('gpqk,qgpd->kgd', probs_bf, dout_f32)
    row_dot = jnp.sum(soft_probs * d_probs, axis=-1, keepdims=True)
    d_scores = (soft_probs * (d_probs - row_dot) * score_scale).astype(jnp.bfloat16).astype(jnp.float32)
    d_query = jnp.einsum('gpqk,kgd->qgpd', d_scores, k_row)
    d_key = jnp.einsum('gpqk,qgpd->kgd', d_scores, q_row)
    d_qkv = jnp.concatenate([d_query, d_key[:, :, None], d_val[:, :, None]], axis=2)
    return attn_out, d_qkv.astype(jnp.bfloat16)


def reference(tokens_in, ln_gain, ln_bias, w_qkv, w_out, w_up, w_down, grad_out):
    tok_count = GROUP_ROWS * SEQ_LEN
    x_flat = tokens_in.reshape(tok_count, DMODEL).astype(jnp.float32)
    dy_flat = grad_out.reshape(tok_count, DMODEL)
    centered = x_flat - jnp.mean(x_flat, axis=-1, keepdims=True)
    inv_std = lax.rsqrt(jnp.mean(centered * centered, axis=-1, keepdims=True) + LN_EPS)
    x_hat = centered * inv_std
    normed = (x_hat * ln_gain + ln_bias).astype(jnp.bfloat16)
    w_qkv_flat = w_qkv.reshape(DMODEL, KV_HEADS * GROUP_COLS)
    qkv_proj = jnp.dot(normed, w_qkv_flat, preferred_element_type=jnp.float32).astype(jnp.bfloat16)
    d_attn = jnp.dot(dy_flat, w_out.T, preferred_element_type=jnp.float32).astype(jnp.bfloat16)
    attn_out, d_qkv = lax.map(attend_row, (qkv_proj.reshape(GROUP_ROWS, SEQ_LEN, KV_HEADS, Q_PER_GROUP + 2, HEAD_DIM), d_attn.reshape(GROUP_ROWS, SEQ_LEN, KV_HEADS, Q_PER_GROUP, HEAD_DIM)))
    attn_flat = attn_out.reshape(tok_count, Q_HEADS * HEAD_DIM)
    d_qkv_flat = d_qkv.reshape(tok_count, KV_HEADS * GROUP_COLS)
    hidden = jnp.dot(normed, w_up, preferred_element_type=jnp.float32)
    gauss_cdf = 0.5 * (1.0 + lax.erf(hidden * GELU_COEF))
    gelu_out = (hidden * gauss_cdf).astype(jnp.bfloat16)
    d_act = jnp.dot(dy_flat, w_down.T, preferred_element_type=jnp.float32)
    d_hidden = (d_act * (gauss_cdf + hidden * PDF_COEF * jnp.exp(-0.5 * hidden * hidden))).astype(jnp.bfloat16)
    grad_qkv = jnp.dot(normed.T, d_qkv_flat, preferred_element_type=jnp.float32).astype(jnp.bfloat16).reshape(DMODEL, KV_HEADS, GROUP_COLS)
    grad_wout = jnp.dot(attn_flat.T, dy_flat, preferred_element_type=jnp.float32).astype(jnp.bfloat16)
    grad_up = jnp.dot(normed.T, d_hidden, preferred_element_type=jnp.float32).astype(jnp.bfloat16)
    grad_down = jnp.dot(gelu_out.T, dy_flat, preferred_element_type=jnp.float32).astype(jnp.bfloat16)
    d_norm = jnp.dot(d_qkv_flat, w_qkv_flat.T, preferred_element_type=jnp.float32) + jnp.dot(d_hidden, w_up.T, preferred_element_type=jnp.float32)
    d_hat = d_norm * ln_gain
    grad_x = inv_std * (d_hat - jnp.mean(d_hat, axis=-1, keepdims=True) - x_hat * jnp.mean(d_hat * x_hat, axis=-1, keepdims=True))
    grad_in = (dy_flat.astype(jnp.float32) + grad_x).astype(jnp.bfloat16).reshape(GROUP_ROWS, SEQ_LEN, DMODEL)
    return (grad_in, grad_qkv, grad_wout, grad_up, grad_down)
```

```python
import functools

import jax
import jax.numpy as jnp
from jax import lax
from jax.experimental import pallas as pl
from jax.experimental.pallas import tpu as pltpu
from jax.sharding import PartitionSpec as P

LN_EPS = 1e-5
GELU_COEF = 0.7071067811865476
PDF_COEF = 0.3989422804014327
LOG2E = 1.4426950408889634
CHUNKS = (1, 2, 3, 3, 3)
HEAD = 128
QBLK = 256
FBLK = 256
F32 = jnp.float32
BF16 = jnp.bfloat16


def dot_nn(a, b):
    return lax.dot_general(a, b, (((1,), (0,)), ((), ())), preferred_element_type=F32)


def dot_nt(a, b):
    return lax.dot_general(a, b, (((1,), (1,)), ((), ())), preferred_element_type=F32)


def dot_tn(a, b):
    return lax.dot_general(a, b, (((0,), (0,)), ((), ())), preferred_element_type=F32)


def branch_kernel(x_ref, dy_ref, gain_ref, bias_ref, wqkv_ref, wout_ref, wup_ref, wdown_ref,
                  part_ref, norm_ref, gelu_ref, dhid_ref, dqkv_ref, ao_ref,
                  qkv_s, dattn_s, p_s, ds_s):
    seq_len, width = x_ref.shape
    heads = wout_ref.shape[0] // HEAD
    ffn = wup_ref.shape[1]
    gain = gain_ref[...]
    bias = bias_ref[...]

    def norm_rows(r, carry):
        rows = pl.ds(pl.multiple_of(r * 128, 128), 128)
        x_f32 = x_ref[rows, :].astype(F32)
        centered = x_f32 - jnp.mean(x_f32, axis=-1, keepdims=True)
        inv_std = lax.rsqrt(jnp.mean(centered * centered, axis=-1, keepdims=True) + LN_EPS)
        norm_ref[rows, :] = (centered * inv_std * gain + bias).astype(BF16)
        return carry

    lax.fori_loop(0, seq_len // 128, norm_rows, 0)

    qkv_s[...] = dot_nn(norm_ref[...], wqkv_ref[...]).astype(BF16)
    dattn_s[...] = dot_nt(dy_ref[...], wout_ref[...]).astype(BF16)

    scale = HEAD ** -0.5
    tri = lax.broadcasted_iota(jnp.int32, (QBLK, QBLK), 0) >= lax.broadcasted_iota(jnp.int32, (QBLK, QBLK), 1)
    nq = seq_len // QBLK
    for h in range(heads):
        base = h * 3 * HEAD
        for i in range(nq):
            rows = slice(i * QBLK, (i + 1) * QBLK)
            span = (i + 1) * QBLK
            q = qkv_s[rows, base:base + HEAD]
            k = qkv_s[:span, base + HEAD:base + 2 * HEAD]
            v = qkv_s[:span, base + 2 * HEAD:base + 3 * HEAD]
            do = dattn_s[rows, h * HEAD:(h + 1) * HEAD]
            s = dot_nt(q, k) * (scale * LOG2E)
            diag = jnp.where(tri, s[:, i * QBLK:], -1e30)
            s = diag if i == 0 else jnp.concatenate([s[:, :i * QBLK], diag], axis=1)
            e = jnp.exp2(s - jnp.max(s, axis=-1, keepdims=True))
            p = e * (1.0 / jnp.sum(e, axis=-1, keepdims=True))
            pb = p.astype(BF16)
            p_s[rows, :span] = pb
            ao_ref[rows, h * HEAD:(h + 1) * HEAD] = dot_nn(pb, v).astype(BF16)
            dp = dot_nt(do, v)
            delta = jnp.sum(p * dp, axis=-1, keepdims=True)
            ds = (p * (dp - delta) * scale).astype(BF16)
            ds_s[rows, :span] = ds
            dqkv_ref[rows, base:base + HEAD] = dot_nn(ds, k).astype(BF16)
        for j in range(nq):
            cols = slice(j * QBLK, (j + 1) * QBLK)
            low = slice(j * QBLK, seq_len)
            dqkv_ref[cols, base + HEAD:base + 2 * HEAD] = dot_tn(ds_s[low, cols], qkv_s[low, base:base + HEAD]).astype(BF16)
            dqkv_ref[cols, base + 2 * HEAD:base + 3 * HEAD] = dot_tn(p_s[low, cols], dattn_s[low, h * HEAD:(h + 1) * HEAD]).astype(BF16)

    def ffn_block(j, carry):
        cols = pl.ds(pl.multiple_of(j * FBLK, FBLK), FBLK)
        hidden = dot_nn(norm_ref[...], wup_ref[:, cols])
        d_act = dot_nt(dy_ref[...], wdown_ref[cols, :])
        cdf = 0.5 * (1.0 + lax.erf(hidden * GELU_COEF))
        gelu_ref[:, cols] = (hidden * cdf).astype(BF16)
        dhid_ref[:, cols] = (d_act * (cdf + hidden * PDF_COEF * jnp.exp(-0.5 * hidden * hidden))).astype(BF16)
        return carry

    lax.fori_loop(0, ffn // FBLK, ffn_block, 0)

    def part_block(j, carry):
        cols = pl.ds(pl.multiple_of(j * 512, 512), 512)
        total = dot_nt(dqkv_ref[...], wqkv_ref[cols, :]) + dot_nt(dhid_ref[...], wup_ref[cols, :])
        part_ref[:, cols] = total.astype(BF16)
        return carry

    lax.fori_loop(0, width // 512, part_block, 0)


def branch_call(tokens, grad_out, gain, bias, wqkv, wout, wup, wdown, first, count, kept, deps):
    num_rows, seq_len, width = tokens.shape
    qkv_w, o_w, ffn = wqkv.shape[1], wout.shape[0], wup.shape[1]

    def seq_in(w):
        return pl.BlockSpec((None, seq_len, w), lambda s: (first + s, 0, 0))

    def whole(a):
        return pl.BlockSpec(a.shape, lambda s: (0, 0), pipeline_mode=pl.Buffered(1))

    tok = count * seq_len
    widths = (width, ffn, ffn, qkv_w, o_w)
    flops = 2 * tok * (width * (2 * qkv_w + o_w + 3 * ffn)) + 12 * tok * seq_len * o_w
    kept = tuple(kept or ())
    extra = len(kept) + len(deps)

    def body(*refs):
        branch_kernel(*refs[:8], *refs[8 + extra:])

    outs = pl.pallas_call(
        body,
        grid=(count,),
        in_specs=[seq_in(width), seq_in(width)] + [whole(a) for a in (gain, bias, wqkv, wout, wup, wdown)] + [pl.BlockSpec(memory_space=pl.ANY)] * extra,
        out_specs=[pl.BlockSpec((seq_len, width), lambda s: (s, 0))] + [pl.BlockSpec((seq_len, w), lambda s: (first + s, 0)) for w in widths],
        out_shape=[jax.ShapeDtypeStruct((tok, width), BF16)] + [jax.ShapeDtypeStruct((num_rows * seq_len, w), BF16) for w in widths],
        input_output_aliases={8 + i: 1 + i for i in range(len(kept))},
        scratch_shapes=[
            pltpu.VMEM((seq_len, qkv_w), BF16),
            pltpu.VMEM((seq_len, o_w), BF16),
            pltpu.VMEM((seq_len, seq_len), BF16),
            pltpu.VMEM((seq_len, seq_len), BF16),
        ],
        compiler_params=pltpu.CompilerParams(dimension_semantics=('arbitrary',), vmem_limit_bytes=63 * 1024 * 1024),
        cost_estimate=pl.CostEstimate(flops=flops, bytes_accessed=tok * 2 * (3 * width + sum(widths)), transcendentals=0),
        name='branch',
    )(tokens, grad_out, gain, bias, wqkv, wout, wup, wdown, *kept, *deps)
    return outs[0], outs[1:]


def finish_kernel(me_ref, total_ref, x_ref, dy_ref, gain_ref, out_ref):
    x_f32 = x_ref[...].astype(F32)
    centered = x_f32 - jnp.mean(x_f32, axis=-1, keepdims=True)
    inv_std = lax.rsqrt(jnp.mean(centered * centered, axis=-1, keepdims=True) + LN_EPS)
    x_hat = centered * inv_std
    d_hat = total_ref[...].astype(F32) * gain_ref[...]
    grad_x = inv_std * (d_hat - jnp.mean(d_hat, axis=-1, keepdims=True) - x_hat * jnp.mean(d_hat * x_hat, axis=-1, keepdims=True))
    out_ref[...] = (dy_ref[...].astype(F32) + grad_x).astype(BF16)


def finish_call(me, total, x_flat, dy_flat, gain, first_row, deps):
    own, width = total.shape
    blk = next(b for b in (192, 128, 96, 64, 32, 16) if own % b == 0 and first_row % b == 0)
    steps, base = own // blk, first_row // blk

    def body(me_ref, total_ref, x_ref, dy_ref, gain_ref, *rest):
        finish_kernel(me_ref, total_ref, x_ref, dy_ref, gain_ref, rest[-1])

    return pl.pallas_call(
        body,
        grid_spec=pltpu.PrefetchScalarGridSpec(
            num_scalar_prefetch=1,
            grid=(steps,),
            in_specs=[
                pl.BlockSpec((blk, width), lambda i, me_ref: (i, 0)),
                pl.BlockSpec((blk, width), lambda i, me_ref: (base + me_ref[0] * steps + i, 0)),
                pl.BlockSpec((blk, width), lambda i, me_ref: (base + me_ref[0] * steps + i, 0)),
                pl.BlockSpec((1, width), lambda i, me_ref: (0, 0)),
            ] + [pl.BlockSpec(memory_space=pl.ANY)] * len(deps),
            out_specs=pl.BlockSpec((blk, width), lambda i, me_ref: (i, 0)),
        ),
        out_shape=jax.ShapeDtypeStruct((own, width), BF16),
        compiler_params=pltpu.CompilerParams(dimension_semantics=('arbitrary',)),
        cost_estimate=pl.CostEstimate(flops=20 * own * width, bytes_accessed=own * width * 8, transcendentals=0),
        name='finish',
    )(me, total, x_flat, dy_flat, gain, *deps)


def weight_call(pairs, deps, blk=1536):
    arrays = []
    for pair in pairs:
        for a in pair:
            if not any(a is other for other in arrays):
                arrays.append(a)
    slots = [tuple(next(i for i, o in enumerate(arrays) if o is a) for a in pair) for pair in pairs]
    tok = arrays[0].shape[0]
    n, m = len(arrays), len(pairs)

    def body(*refs):
        ins, outs, accs = refs[:n], refs[n + len(deps):n + len(deps) + m], refs[n + len(deps) + m:]
        step = pl.program_id(0)

        @pl.when(step == 0)
        def _():
            for acc in accs:
                acc[...] = jnp.zeros_like(acc)

        for (ia, ib), acc in zip(slots, accs):
            a_ref, b_ref = ins[ia], ins[ib]

            def rows_block(r, carry):
                rows = pl.ds(pl.multiple_of(r * 256, 256), 256)
                acc[rows, :] += dot_tn(a_ref[:, rows], b_ref[...])
                return carry

            lax.fori_loop(0, acc.shape[0] // 256, rows_block, 0)

        @pl.when(step == pl.num_programs(0) - 1)
        def _():
            for out, acc in zip(outs, accs):
                out[...] = acc[...].astype(BF16)

    shapes = [(a.shape[1], b.shape[1]) for a, b in pairs]
    flops = sum(2 * tok * x * y for x, y in shapes)
    return pl.pallas_call(
        body,
        grid=(tok // blk,),
        in_specs=[pl.BlockSpec((blk, a.shape[1]), lambda s: (s, 0)) for a in arrays] + [pl.BlockSpec(memory_space=pl.ANY)] * len(deps),
        out_specs=[pl.BlockSpec(shape, lambda s: (0, 0), pipeline_mode=pl.Buffered(1)) for shape in shapes],
        out_shape=[jax.ShapeDtypeStruct(shape, BF16) for shape in shapes],
        scratch_shapes=[pltpu.VMEM(shape, F32) for shape in shapes],
        compiler_params=pltpu.CompilerParams(dimension_semantics=('arbitrary',), vmem_limit_bytes=63 * 1024 * 1024),
        cost_estimate=pl.CostEstimate(flops=flops, bytes_accessed=sum(2 * a.size for a in arrays), transcendentals=0),
        name='weights',
    )(*arrays, *deps)


def solution(mesh):
    row_spec = P('dp', None, None)
    in_specs = (row_spec, P(None), P(None), P(None, 'tp', None), P('tp', None), P(None, 'tp'), P('tp', None), row_spec)
    out_specs = (row_spec, P('dp', 'tp', None), P(('dp', 'tp'), None), P('dp', 'tp'), P(('dp', 'tp'), None))
    ntp = mesh.shape['tp']

    def device_step(tokens, ln_gain, ln_bias, w_qkv, w_out, w_up, w_down, grad_out):
        num_rows, seq_len, width = tokens.shape
        groups, per_group = w_qkv.shape[1:]
        wqkv = w_qkv.reshape(width, groups * per_group)
        gain, bias = ln_gain.reshape(1, width), ln_bias.reshape(1, width)
        counts = [num_rows * share // sum(CHUNKS) for share in CHUNKS]
        firsts = [sum(counts[:c]) for c in range(len(counts))]
        x_flat = tokens.reshape(num_rows * seq_len, width)
        dy_flat = grad_out.reshape(num_rows * seq_len, width)
        me = lax.axis_index('tp').astype(jnp.int32).reshape(1)
        totals, finished, gathered = [], [], []

        def finish(deps):
            c = len(finished)
            finished.append(finish_call(me, totals[c], x_flat, dy_flat, gain, firsts[c] * seq_len, deps))
            gathered.append(lax.all_gather(finished[c], 'tp', axis=0, tiled=True))

        kept = None
        for c, count in enumerate(counts):
            part, kept = branch_call(tokens, grad_out, gain, bias, wqkv, w_out, w_up, w_down, firsts[c], count, kept, finished[-1:] + (gathered[c - 3:c - 2] if c >= 3 else []))
            totals.append(lax.psum_scatter(part, 'tp', scatter_dimension=0, tiled=True))
            if 1 <= c < len(counts) - 1:
                finish([kept[-1]])
        normed, gelu, dhid, dqkv, ao = kept
        (g_out,) = weight_call([(ao, dy_flat)], finished[-1:])
        finish([g_out])
        (g_down,) = weight_call([(gelu, dy_flat)], finished[-1:])
        finish([g_down])
        g_up, g_qkv = weight_call([(normed, dhid), (normed, dqkv)], finished[-1:])
        grad_in = jnp.concatenate(gathered, axis=0).reshape(tokens.shape)
        return grad_in, g_qkv.reshape(width, groups, per_group), g_out, g_up, g_down

    return jax.shard_map(device_step, mesh=mesh, in_specs=in_specs, out_specs=out_specs, check_vma=False)
```

```python
import functools

import jax
import jax.numpy as jnp
from jax import lax
from jax.experimental import pallas as pl
from jax.experimental.pallas import tpu as pltpu
from jax.sharding import PartitionSpec as P

LN_EPS = 1e-5
GELU_COEF = 0.7071067811865476
PDF_COEF = 0.3989422804014327
LOG2E = 1.4426950408889634
CHUNKS = (4, 10, 14, 12, 8)
HEAD = 128
QBLK = 256
FBLK = 256
ROW_BLOCK = 512
F32 = jnp.float32
BF16 = jnp.bfloat16


def dot_nn(a, b):
    return lax.dot_general(a, b, (((1,), (0,)), ((), ())), preferred_element_type=F32)


def dot_nt(a, b):
    return lax.dot_general(a, b, (((1,), (1,)), ((), ())), preferred_element_type=F32)


def dot_tn(a, b):
    return lax.dot_general(a, b, (((0,), (0,)), ((), ())), preferred_element_type=F32)


def branch_kernel(x_ref, dy_ref, gain_ref, bias_ref, wqkv_ref, wout_ref, wup_ref, wdown_ref,
                  part_ref, norm_ref, gelu_ref, dhid_ref, dqkv_ref, ao_ref,
                  qkv_s, dattn_s, p_s, ds_s):
    seq_len, width = x_ref.shape
    heads = wout_ref.shape[0] // HEAD
    ffn = wup_ref.shape[1]
    gain = gain_ref[...]
    bias = bias_ref[...]

    def norm_rows(r, carry):
        rows = pl.ds(pl.multiple_of(r * 128, 128), 128)
        x_f32 = x_ref[rows, :].astype(F32)
        centered = x_f32 - jnp.mean(x_f32, axis=-1, keepdims=True)
        inv_std = lax.rsqrt(jnp.mean(centered * centered, axis=-1, keepdims=True) + LN_EPS)
        norm_ref[rows, :] = (centered * inv_std * gain + bias).astype(BF16)
        return carry

    lax.fori_loop(0, seq_len // 128, norm_rows, 0)

    qkv_s[...] = dot_nn(norm_ref[...], wqkv_ref[...]).astype(BF16)
    dattn_s[...] = dot_nt(dy_ref[...], wout_ref[...]).astype(BF16)

    scale = HEAD ** -0.5
    tri = lax.broadcasted_iota(jnp.int32, (QBLK, QBLK), 0) >= lax.broadcasted_iota(jnp.int32, (QBLK, QBLK), 1)
    nq = seq_len // QBLK
    for h in range(heads):
        base = h * 3 * HEAD
        for i in range(nq):
            rows = slice(i * QBLK, (i + 1) * QBLK)
            span = (i + 1) * QBLK
            q = qkv_s[rows, base:base + HEAD]
            k = qkv_s[:span, base + HEAD:base + 2 * HEAD]
            v = qkv_s[:span, base + 2 * HEAD:base + 3 * HEAD]
            do = dattn_s[rows, h * HEAD:(h + 1) * HEAD]
            s = dot_nt(q, k) * (scale * LOG2E)
            diag = jnp.where(tri, s[:, i * QBLK:], -1e30)
            s = diag if i == 0 else jnp.concatenate([s[:, :i * QBLK], diag], axis=1)
            e = jnp.exp2(s - jnp.max(s, axis=-1, keepdims=True))
            p = e * (1.0 / jnp.sum(e, axis=-1, keepdims=True))
            pb = p.astype(BF16)
            p_s[rows, :span] = pb
            ao_ref[rows, h * HEAD:(h + 1) * HEAD] = dot_nn(pb, v).astype(BF16)
            dp = dot_nt(do, v)
            delta = jnp.sum(p * dp, axis=-1, keepdims=True)
            ds = (p * (dp - delta) * scale).astype(BF16)
            ds_s[rows, :span] = ds
            dqkv_ref[rows, base:base + HEAD] = dot_nn(ds, k).astype(BF16)
        for j in range(nq):
            cols = slice(j * QBLK, (j + 1) * QBLK)
            low = slice(j * QBLK, seq_len)
            dqkv_ref[cols, base + HEAD:base + 2 * HEAD] = dot_tn(ds_s[low, cols], qkv_s[low, base:base + HEAD]).astype(BF16)
            dqkv_ref[cols, base + 2 * HEAD:base + 3 * HEAD] = dot_tn(p_s[low, cols], dattn_s[low, h * HEAD:(h + 1) * HEAD]).astype(BF16)

    def ffn_block(j, carry):
        cols = pl.ds(pl.multiple_of(j * FBLK, FBLK), FBLK)
        hidden = dot_nn(norm_ref[...], wup_ref[:, cols])
        d_act = dot_nt(dy_ref[...], wdown_ref[cols, :])
        cdf = 0.5 * (1.0 + lax.erf(hidden * GELU_COEF))
        gelu_ref[:, cols] = (hidden * cdf).astype(BF16)
        dhid_ref[:, cols] = (d_act * (cdf + hidden * PDF_COEF * jnp.exp(-0.5 * hidden * hidden))).astype(BF16)
        return carry

    lax.fori_loop(0, ffn // FBLK, ffn_block, 0)

    def part_block(j, carry):
        cols = pl.ds(pl.multiple_of(j * 512, 512), 512)
        total = dot_nt(dqkv_ref[...], wqkv_ref[cols, :]) + dot_nt(dhid_ref[...], wup_ref[cols, :])
        part_ref[:, cols] = total.astype(BF16)
        return carry

    lax.fori_loop(0, width // 512, part_block, 0)


def branch_call(tokens, grad_out, gain, bias, wqkv, wout, wup, wdown, first, count, kept, deps):
    num_rows, seq_len, width = tokens.shape
    qkv_w, o_w, ffn = wqkv.shape[1], wout.shape[0], wup.shape[1]

    def seq_in(w):
        return pl.BlockSpec((None, seq_len, w), lambda s: (first + s, 0, 0))

    def whole(a):
        return pl.BlockSpec(a.shape, lambda s: (0, 0), pipeline_mode=pl.Buffered(1))

    tok = count * seq_len
    widths = (width, ffn, ffn, qkv_w, o_w)
    flops = 2 * tok * (width * (2 * qkv_w + o_w + 3 * ffn)) + 12 * tok * seq_len * o_w
    kept = tuple(kept or ())
    extra = len(kept) + len(deps)

    def body(*refs):
        branch_kernel(*refs[:8], *refs[8 + extra:])

    outs = pl.pallas_call(
        body,
        grid=(count,),
        in_specs=[seq_in(width), seq_in(width)] + [whole(a) for a in (gain, bias, wqkv, wout, wup, wdown)] + [pl.BlockSpec(memory_space=pl.ANY)] * extra,
        out_specs=[pl.BlockSpec((seq_len, width), lambda s: (s, 0))] + [pl.BlockSpec((seq_len, w), lambda s: (first + s, 0)) for w in widths],
        out_shape=[jax.ShapeDtypeStruct((tok, width), BF16)] + [jax.ShapeDtypeStruct((num_rows * seq_len, w), BF16) for w in widths],
        input_output_aliases={8 + i: 1 + i for i in range(len(kept))},
        scratch_shapes=[
            pltpu.VMEM((seq_len, qkv_w), BF16),
            pltpu.VMEM((seq_len, o_w), BF16),
            pltpu.VMEM((seq_len, seq_len), BF16),
            pltpu.VMEM((seq_len, seq_len), BF16),
        ],
        compiler_params=pltpu.CompilerParams(dimension_semantics=('arbitrary',), vmem_limit_bytes=63 * 1024 * 1024),
        cost_estimate=pl.CostEstimate(flops=flops, bytes_accessed=tok * 2 * (3 * width + sum(widths)), transcendentals=0),
        name='branch',
    )(tokens, grad_out, gain, bias, wqkv, wout, wup, wdown, *kept, *deps)
    return outs[0], outs[1:]


def finish_kernel(me_ref, total_ref, x_ref, dy_ref, gain_ref, out_ref):
    x_f32 = x_ref[...].astype(F32)
    centered = x_f32 - jnp.mean(x_f32, axis=-1, keepdims=True)
    inv_std = lax.rsqrt(jnp.mean(centered * centered, axis=-1, keepdims=True) + LN_EPS)
    x_hat = centered * inv_std
    d_hat = total_ref[...].astype(F32) * gain_ref[...]
    grad_x = inv_std * (d_hat - jnp.mean(d_hat, axis=-1, keepdims=True) - x_hat * jnp.mean(d_hat * x_hat, axis=-1, keepdims=True))
    out_ref[...] = (dy_ref[...].astype(F32) + grad_x).astype(BF16)


def finish_call(me, total, x_flat, dy_flat, gain, first_row, deps):
    own, width = total.shape
    blk = next(b for b in (192, 128, 96, 64, 32, 16) if own % b == 0 and first_row % b == 0)
    steps, base = own // blk, first_row // blk

    def body(me_ref, total_ref, x_ref, dy_ref, gain_ref, *rest):
        finish_kernel(me_ref, total_ref, x_ref, dy_ref, gain_ref, rest[-1])

    return pl.pallas_call(
        body,
        grid_spec=pltpu.PrefetchScalarGridSpec(
            num_scalar_prefetch=1,
            grid=(steps,),
            in_specs=[
                pl.BlockSpec((blk, width), lambda i, me_ref: (i, 0)),
                pl.BlockSpec((blk, width), lambda i, me_ref: (base + me_ref[0] * steps + i, 0)),
                pl.BlockSpec((blk, width), lambda i, me_ref: (base + me_ref[0] * steps + i, 0)),
                pl.BlockSpec((1, width), lambda i, me_ref: (0, 0)),
            ] + [pl.BlockSpec(memory_space=pl.ANY)] * len(deps),
            out_specs=pl.BlockSpec((blk, width), lambda i, me_ref: (i, 0)),
        ),
        out_shape=jax.ShapeDtypeStruct((own, width), BF16),
        compiler_params=pltpu.CompilerParams(dimension_semantics=('arbitrary',)),
        cost_estimate=pl.CostEstimate(flops=20 * own * width, bytes_accessed=own * width * 8, transcendentals=0),
        name='finish',
    )(me, total, x_flat, dy_flat, gain, *deps)


def weight_call(pairs, deps, blk=1536):
    arrays = []
    for pair in pairs:
        for a in pair:
            if not any(a is other for other in arrays):
                arrays.append(a)
    slots = [tuple(next(i for i, o in enumerate(arrays) if o is a) for a in pair) for pair in pairs]
    tok = arrays[0].shape[0]
    n, m = len(arrays), len(pairs)

    def body(*refs):
        ins, outs, accs = refs[:n], refs[n + len(deps):n + len(deps) + m], refs[n + len(deps) + m:]
        step = pl.program_id(0)

        @pl.when(step == 0)
        def _():
            for acc in accs:
                acc[...] = jnp.zeros_like(acc)

        for (ia, ib), acc in zip(slots, accs):
            a_ref, b_ref = ins[ia], ins[ib]

            size = min(ROW_BLOCK, acc.shape[0])

            def rows_block(r, carry, a_ref=a_ref, b_ref=b_ref, acc=acc, size=size):
                rows = pl.ds(pl.multiple_of(r * size, size), size)
                acc[rows, :] += dot_tn(a_ref[:, rows], b_ref[...])
                return carry

            lax.fori_loop(0, acc.shape[0] // size, rows_block, 0)

        @pl.when(step == pl.num_programs(0) - 1)
        def _():
            for out, acc in zip(outs, accs):
                out[...] = acc[...].astype(BF16)

    shapes = [(a.shape[1], b.shape[1]) for a, b in pairs]
    flops = sum(2 * tok * x * y for x, y in shapes)
    return pl.pallas_call(
        body,
        grid=(tok // blk,),
        in_specs=[pl.BlockSpec((blk, a.shape[1]), lambda s: (s, 0)) for a in arrays] + [pl.BlockSpec(memory_space=pl.ANY)] * len(deps),
        out_specs=[pl.BlockSpec(shape, lambda s: (0, 0), pipeline_mode=pl.Buffered(1)) for shape in shapes],
        out_shape=[jax.ShapeDtypeStruct(shape, BF16) for shape in shapes],
        scratch_shapes=[pltpu.VMEM(shape, F32) for shape in shapes],
        compiler_params=pltpu.CompilerParams(dimension_semantics=('arbitrary',), vmem_limit_bytes=63 * 1024 * 1024),
        cost_estimate=pl.CostEstimate(flops=flops, bytes_accessed=sum(2 * a.size for a in arrays), transcendentals=0),
        name='weights',
    )(*arrays, *deps)


def solution(mesh):
    row_spec = P('dp', None, None)
    in_specs = (row_spec, P(None), P(None), P(None, 'tp', None), P('tp', None), P(None, 'tp'), P('tp', None), row_spec)
    out_specs = (row_spec, P('dp', 'tp', None), P(('dp', 'tp'), None), P('dp', 'tp'), P(('dp', 'tp'), None))
    ntp = mesh.shape['tp']

    def device_step(tokens, ln_gain, ln_bias, w_qkv, w_out, w_up, w_down, grad_out):
        num_rows, seq_len, width = tokens.shape
        groups, per_group = w_qkv.shape[1:]
        wqkv = w_qkv.reshape(width, groups * per_group)
        gain, bias = ln_gain.reshape(1, width), ln_bias.reshape(1, width)
        counts = [num_rows * share // sum(CHUNKS) for share in CHUNKS]
        firsts = [sum(counts[:c]) for c in range(len(counts))]
        x_flat = tokens.reshape(num_rows * seq_len, width)
        dy_flat = grad_out.reshape(num_rows * seq_len, width)
        me = lax.axis_index('tp').astype(jnp.int32).reshape(1)
        totals, finished, gathered = [], [], []

        def finish(deps):
            c = len(finished)
            finished.append(finish_call(me, totals[c], x_flat, dy_flat, gain, firsts[c] * seq_len, deps))
            gathered.append(lax.all_gather(finished[c], 'tp', axis=0, tiled=True))

        kept = None
        for c, count in enumerate(counts):
            part, kept = branch_call(tokens, grad_out, gain, bias, wqkv, w_out, w_up, w_down, firsts[c], count, kept, finished[-1:] + (gathered[c - 3:c - 2] if c >= 3 else []))
            totals.append(lax.psum_scatter(part, 'tp', scatter_dimension=0, tiled=True))
            if 1 <= c < len(counts) - 1:
                finish([kept[-1]])
        normed, gelu, dhid, dqkv, ao = kept
        (g_out,) = weight_call([(ao, dy_flat)], finished[-1:])
        finish([g_out])
        (g_down,) = weight_call([(gelu, dy_flat)], finished[-1:])
        finish([g_down])
        g_up, g_qkv = weight_call([(normed, dhid), (normed, dqkv)], finished[-1:])
        grad_in = jnp.concatenate(gathered, axis=0).reshape(tokens.shape)
        return grad_in, g_qkv.reshape(width, groups, per_group), g_out, g_up, g_down

    return jax.shard_map(device_step, mesh=mesh, in_specs=in_specs, out_specs=out_specs, check_vma=False)
```
